32 devices in a mesh: groups: 2 (over x), tp: 16 (over z, y, core).
Axes of the slice: x: 2, y: 2, z: 4, core: 2. Of those that a mesh axis runs over, the one named last changes fastest.
Arguments:
- queries: bfloat16 [4, 4096, 4096], P('groups', 'tp'), parts along dimension 0, may hold values from -162 to 162
- keys: bfloat16 [4, 4096, 2048], P('groups', 'tp'), parts along dimension 0, may hold values from -6 to 6
- values: bfloat16 [4, 4096, 2048], P('groups', 'tp'), parts along dimension 0, may hold values from -6 to 6
- lengths: int32 [4], P('groups'), parts along dimension 0, may hold values from 1024 to 4096
Outputs:
- attended: bfloat16 [4, 4096, 4096], P('groups', 'tp'), parts along dimension 0
The draws below stay inside these ranges and needn't reach their ends.
There are 2 independent parts, one for each index of `groups`. The reference program is written for one: setup_inputs(seed, part) draws one part's arguments, and reference() takes and returns one part's arrays. A program takes and returns all parts, laid end to end along the dimension named above; each array names one. Nothing has to cross between parts.
All inputs are finite; a program needn't handle non-finite values.
Results may differ from the reference program's by a relative error of at most 0.0085.
Values may be sent and summed in bfloat16 or wider, within the bound.
A program may use at most 256 MiB of HBM per device.

```python
import jax
import jax.numpy as jnp
from jax import lax

HEADS = 32
KVH = 16
HD = 128
SEQS = 2
LEN = 4096


def key_field(key):
    sub = jax.random.fold_in(key, 11)
    field = jnp.clip(jax.random.normal(sub, (SEQS, LEN, KVH * HD), jnp.float32), -6.0, 6.0)
    return field


def draw_keys(key, part):
    return key_field(key).astype(jnp.bfloat16)


def draw_queries(key, part):
    field = key_field(key).reshape(SEQS, LEN, KVH, HD)
    subkeys = jax.random.split(jax.random.fold_in(key, 23), 6)
    shape = (SEQS, LEN, HEADS)
    base = jnp.clip(jax.random.normal(subkeys[0], (SEQS, LEN, HEADS, HD), jnp.float32), -6.0, 6.0)
    share = 0.125
    places = jnp.arange(LEN, dtype=jnp.int32)
    reach = jnp.minimum(places + 1, max(LEN // 4, 1))[None, :, None]
    first = jax.random.randint(subkeys[1], shape, 0, reach)
    offset = jax.random.randint(subkeys[2], shape, 0, jnp.maximum(reach - 1, 1))
    second = (first + 1 + offset) % reach
    lead = jax.random.uniform(subkeys[3], shape, jnp.float32, 100.0, 150.0) * (12.0 / HD)
    ratio = jax.random.uniform(subkeys[4], shape, jnp.float32, 0.65, 0.85)
    chosen = jax.random.uniform(subkeys[5], shape, jnp.float32) < share
    seq_index = jnp.arange(SEQS, dtype=jnp.int32)[:, None, None]
    head_index = (jnp.arange(HEADS, dtype=jnp.int32) // 2)[None, None, :]
    pick_first = field[seq_index, first, head_index]
    pick_second = field[seq_index, second, head_index]
    aligned = lead[..., None] * pick_first + (lead * ratio)[..., None] * pick_second
    result = base + jnp.where(chosen[..., None], aligned, 0.0)
    return result.reshape(SEQS, LEN, HEADS * HD).astype(jnp.bfloat16)


def level_of(own_key, shape, cuts, low, top_value):
    level = 1.0
    for dim, blocks in cuts:
        heights = jax.random.uniform(jax.random.fold_in(jax.random.fold_in(own_key, 6), dim), (blocks,), jnp.float32, low / len(cuts), top_value / len(cuts))
        level = level * jnp.repeat(jnp.exp(heights), shape[dim] // blocks).reshape((-1,) + (1,) * (len(shape) - 1 - dim))
    return level


def normal_values(key, shape, scale, most, pieces=(), kind=jnp.bfloat16):
    values = scale * jax.random.normal(key, shape, jnp.float32)
    if pieces:
        values = values * level_of(key, shape, pieces, -0.22, 0.18)
    return jnp.clip(values, -most, most).astype(kind)


def setup_inputs(seed: int = 0, part: int = 0) -> dict:
    key_of = jax.random.split(jax.random.key(seed), 5)
    part_splits = jax.random.split(jax.random.fold_in(key_of[4], part), 5)
    queries = draw_queries(jax.random.fold_in(jax.random.fold_in(key_of[4], part), 71), part)
    keys = draw_keys(jax.random.fold_in(jax.random.fold_in(key_of[4], part), 71), part)
    values = normal_values(part_splits[2], (SEQS, LEN, KVH * HD), 1.0, 6.0, ((1, 16),))
    lengths = jax.random.randint(part_splits[3], (SEQS,), LEN // 4, LEN + 1).astype(jnp.int32)
    return dict(queries=queries, keys=keys, values=values, lengths=lengths)


query_scale = 144.0 ** -0.5
soft_cap = 50.0


def one_head(operands):
    head_q, head_k, head_v, valid = operands
    score = jnp.dot(head_q.astype(jnp.float32), head_k.astype(jnp.float32).T) * query_scale
    capped = soft_cap * jnp.tanh(score / soft_cap)
    places = jnp.arange(LEN)
    allowed = (places[None, :] <= places[:, None]) & (places[None, :] < valid)
    weight = jnp.where(allowed, jnp.exp(capped), 0.0)
    total = jnp.sum(weight, axis=1)
    rounded = weight.astype(jnp.bfloat16)
    mixed = jnp.dot(rounded.astype(jnp.float32), head_v.astype(jnp.float32)) / total[:, None]
    live = places[:, None] < valid
    return jnp.where(live, mixed, 0.0).astype(jnp.bfloat16)


def reference(queries, keys, values, lengths):
    split_q = queries.reshape(SEQS, LEN, HEADS, HD).transpose(0, 2, 1, 3).reshape(SEQS * HEADS, LEN, HD)
    split_k = jnp.repeat(keys.reshape(SEQS, LEN, KVH, HD).transpose(0, 2, 1, 3), 2, axis=1).reshape(SEQS * HEADS, LEN, HD)
    split_v = jnp.repeat(values.reshape(SEQS, LEN, KVH, HD).transpose(0, 2, 1, 3), 2, axis=1).reshape(SEQS * HEADS, LEN, HD)
    valid = jnp.repeat(lengths.astype(jnp.int32), HEADS)
    result = lax.map(one_head, (split_q, split_k, split_v, valid))
    return result.reshape(SEQS, HEADS, LEN, HD).transpose(0, 2, 1, 3).reshape(SEQS, LEN, HEADS * HD)
```

```python
import functools
import math

import jax
import jax.numpy as jnp
from jax import lax
from jax.experimental import pallas as pl
from jax.experimental.pallas import tpu as pltpu
from jax.sharding import PartitionSpec as P

HEADS = 32
KVH = 16
HD = 128
GROUP = HEADS // KVH

SOFT_CAP = 50.0
SCORE_SCALE = 1.0 / (math.sqrt(144.0) * SOFT_CAP)
EXP_SCALE = SOFT_CAP * math.log2(math.e)


def attend_kernel(heads, width, span, length_ref, packed_ref, out_ref, key_ext, total_ref):
    index = pl.program_id(0)
    valid = length_ref[0]
    count = packed_ref.shape[0]
    start = index * width

    @pl.when(index == 0)
    def _():
        key_ext[:, :HD] = packed_ref[:, (heads + 1) * HD :]
        key_ext[:, HD:] = jnp.ones((count, HD), jnp.bfloat16)

    @pl.when(start >= valid)
    def _():
        out_ref[...] = jnp.zeros_like(out_ref)

    @pl.when(start < valid)
    def _():
        rows = pl.ds(pl.multiple_of(start, width), width)
        block_q = jnp.concatenate(
            [packed_ref[rows, h * HD : (h + 1) * HD] for h in range(heads)], axis=0
        )
        total_ref[...] = jnp.zeros_like(total_ref)

        def step(block, masked):
            first = pl.multiple_of(block * span, span)
            keys = packed_ref[pl.ds(first, span), heads * HD : (heads + 1) * HD]
            score = lax.dot_general(
                block_q, keys, (((1,), (1,)), ((), ())), preferred_element_type=jnp.float32
            )
            weight = jnp.exp2(jnp.tanh(score * SCORE_SCALE) * EXP_SCALE)
            if masked:
                shape = (width, span)
                key_pos = first + lax.broadcasted_iota(jnp.int32, shape, 1)
                query_pos = start + lax.broadcasted_iota(jnp.int32, shape, 0)
                allowed = (key_pos <= query_pos) & (key_pos < valid)
                weight = jnp.concatenate(
                    [
                        jnp.where(allowed, weight[h * width : (h + 1) * width], 0.0)
                        for h in range(heads)
                    ],
                    axis=0,
                )
            total_ref[...] += jnp.dot(
                weight.astype(jnp.bfloat16),
                key_ext[pl.ds(first, span), :],
                preferred_element_type=jnp.float32,
            )

        full = jnp.minimum(start + 1, valid) // span
        stop = (jnp.minimum(start + width, valid) + span - 1) // span

        def plain(block, carry):
            step(block, False)
            return carry

        def edge(block, carry):
            step(block, True)
            return carry

        lax.fori_loop(0, full, plain, 0)
        lax.fori_loop(full, stop, edge, 0)
        live = start + lax.broadcasted_iota(jnp.int32, (width, HD), 0) < valid
        for h in range(heads):
            part = slice(h * width, (h + 1) * width)
            mixed = total_ref[part, :HD] / total_ref[part, HD:]
            out_ref[:, h * HD : (h + 1) * HD] = jnp.where(live, mixed, 0.0).astype(jnp.bfloat16)


def attend(packed, valid, heads):
    count = packed.shape[0]
    width = min(256, count)
    span = min(512, count)
    return pl.pallas_call(
        functools.partial(attend_kernel, heads, width, span),
        grid_spec=pltpu.PrefetchScalarGridSpec(
            num_scalar_prefetch=1,
            grid=(count // width,),
            in_specs=[pl.BlockSpec((count, (heads + 2) * HD), lambda i, _: (0, 0))],
            out_specs=pl.BlockSpec((width, heads * HD), lambda i, _: (i, 0)),
            scratch_shapes=[
                pltpu.VMEM((count, 2 * HD), jnp.bfloat16),
                pltpu.VMEM((heads * width, 2 * HD), jnp.float32),
            ],
        ),
        out_shape=jax.ShapeDtypeStruct((count, heads * HD), jnp.bfloat16),
        cost_estimate=pl.CostEstimate(
            flops=4 * heads * count * count * HD,
            bytes_accessed=2 * count * HD * (2 * heads + 2),
            transcendentals=heads * count * count,
        ),
        compiler_params=pltpu.CompilerParams(
            dimension_semantics=("arbitrary",), vmem_limit_bytes=40 * 1024 * 1024
        ),
    )(valid, packed)


def pack_kernel(query_ref, key_ref, value_ref, out_ref):
    out_ref[0, :, : GROUP * HD] = query_ref[0]
    out_ref[0, :, GROUP * HD : (GROUP + 1) * HD] = key_ref[0]
    out_ref[0, :, (GROUP + 1) * HD :] = value_ref[0]


def pack(queries, keys, values, s):
    rows = queries.shape[1]
    size = (GROUP + 2) * HD
    return pl.pallas_call(
        pack_kernel,
        grid=(KVH,),
        in_specs=[
            pl.BlockSpec((1, rows, GROUP * HD), lambda h: (s, 0, h)),
            pl.BlockSpec((1, rows, HD), lambda h: (s, 0, h)),
            pl.BlockSpec((1, rows, HD), lambda h: (s, 0, h)),
        ],
        out_specs=pl.BlockSpec((1, rows, size), lambda h: (h, 0, 0)),
        out_shape=jax.ShapeDtypeStruct((KVH, rows, size), jnp.bfloat16),
        cost_estimate=pl.CostEstimate(
            flops=0, bytes_accessed=4 * KVH * rows * size, transcendentals=0
        ),
    )(queries, keys, values)


def unpack_kernel(*refs):
    out_ref = refs[-1]
    for s, ref in enumerate(refs[:-1]):
        out_ref[s] = ref[0]


def unpack(returned):
    _, rows, size = returned[0].shape
    seqs = len(returned)
    return pl.pallas_call(
        unpack_kernel,
        grid=(KVH,),
        in_specs=[pl.BlockSpec((1, rows, size), lambda h: (h, 0, 0))] * seqs,
        out_specs=pl.BlockSpec((seqs, rows, size), lambda h: (0, 0, h)),
        out_shape=jax.ShapeDtypeStruct((seqs, rows, KVH * size), jnp.bfloat16),
        cost_estimate=pl.CostEstimate(
            flops=0, bytes_accessed=4 * KVH * seqs * rows * size, transcendentals=0
        ),
    )(*returned)


def exchange(array):
    return lax.all_to_all(array, "tp", split_axis=0, concat_axis=0, tiled=True)


def per_device(queries, keys, values, lengths):
    seqs, rows, _ = queries.shape
    devices = lax.axis_size("tp")
    count = devices * rows
    if KVH % devices == 0:
        owned = KVH // devices
        gathered = []
        for s in range(seqs):
            packed = pack(queries, keys, values, s).reshape(devices, owned * rows, -1)
            gathered.append(exchange(packed).reshape(devices, owned, rows, -1))
        returned = []
        for s in range(seqs):
            outs = [
                attend(gathered[s][:, o].reshape(count, -1), lengths[s : s + 1], GROUP)
                for o in range(owned)
            ]
            output = outs[0] if owned == 1 else jnp.stack(outs).reshape(owned, devices, rows, -1)
            if owned > 1:
                output = output.transpose(1, 0, 2, 3)
            back = exchange(output.reshape(devices, owned * rows, GROUP * HD))
            returned.append(back.reshape(KVH, rows, GROUP * HD))
        return unpack(returned)

    pairs = seqs * HEADS
    owned = pairs // devices
    heads_q = queries.reshape(seqs, rows, HEADS, HD)
    heads_k = jnp.repeat(keys.reshape(seqs, rows, KVH, HD), GROUP, axis=2)
    heads_v = jnp.repeat(values.reshape(seqs, rows, KVH, HD), GROUP, axis=2)
    packed = jnp.concatenate([heads_q, heads_k, heads_v], axis=3)
    packed = packed.transpose(0, 2, 1, 3).reshape(devices, owned * rows, 3 * HD)
    gathered = exchange(packed).reshape(devices, owned, rows, 3 * HD)
    outs = []
    for o in range(owned):
        seq = (lax.axis_index("tp") * owned + o) // HEADS
        valid = jnp.sum(jnp.where(jnp.arange(seqs) == seq, lengths, 0))[None]
        outs.append(attend(gathered[:, o].reshape(count, 3 * HD), valid, 1))
    output = jnp.stack(outs).reshape(owned, devices, rows, HD).transpose(1, 0, 2, 3)
    returned = exchange(output.reshape(devices, owned * rows, HD))
    return (
        returned.reshape(seqs, HEADS, rows, HD)
        .transpose(0, 2, 1, 3)
        .reshape(seqs, rows, HEADS * HD)
    )


def solution(mesh):
    placed = (
        P("groups", "tp", None),
        P("groups", "tp", None),
        P("groups", "tp", None),
        P("groups"),
    )
    return jax.shard_map(
        per_device, mesh=mesh, in_specs=placed, out_specs=P("groups", "tp", None), check_vma=False
    )
```

```python
import functools
import math

import jax
import jax.numpy as jnp
from jax import lax
from jax.experimental import pallas as pl
from jax.experimental.pallas import tpu as pltpu
from jax.sharding import PartitionSpec as P


HEADS = 32
KVH = 16
HD = 128
GROUP = HEADS // KVH

SOFT_CAP = 50.0
SCORE_SCALE = 1.0 / (math.sqrt(144.0) * SOFT_CAP)
EXP_SCALE = SOFT_CAP * math.log2(math.e)


def attend_half_kernel(
    width, span, info_ref, query_ref, own_ref, early_ref, out_ref, key_all, value_ext, total_ref
):
    index = pl.program_id(0)
    valid = info_ref[0]
    base = pl.multiple_of(info_ref[1], span)
    blocks, _, rows, _ = own_ref.shape
    part = blocks * rows
    start = base + index * width

    @pl.when((index == 0) & (base < valid))
    def _():
        early = early_ref[...].reshape(part, 2 * HD)
        key_all[:part, :] = early[:, :HD]
        value_ext[:part, :HD] = early[:, HD:]
        own = own_ref[:, 0].reshape(part, 2 * HD)
        key_all[pl.ds(base, part), :] = own[:, :HD]
        value_ext[pl.ds(base, part), :HD] = own[:, HD:]
        value_ext[:, HD:] = jnp.ones((2 * part, HD), jnp.bfloat16)

    attend_block(
        GROUP, width, span, start, valid, query_ref, (0, 0), key_all, value_ext, out_ref, (0,), total_ref
    )


def attend_block(
    heads, width, span, start, valid, query_ref, at_q, key_all, value_ext, out_ref, at_o, total_ref
):
    @pl.when(start >= valid)
    def _():
        out_ref[...] = jnp.zeros_like(out_ref)

    @pl.when(start < valid)
    def _():
        block_q = jnp.concatenate(
            [query_ref[at_q + (slice(None), slice(h * HD, (h + 1) * HD))] for h in range(heads)],
            axis=0,
        )
        total_ref[...] = jnp.zeros_like(total_ref)

        def step(block, masked):
            first = pl.multiple_of(block * span, span)
            score = lax.dot_general(
                block_q,
                key_all[pl.ds(first, span), :],
                (((1,), (1,)), ((), ())),
                preferred_element_type=jnp.float32,
            )
            weight = jnp.exp2(jnp.tanh(score * SCORE_SCALE) * EXP_SCALE)
            if masked:
                shape = (width, span)
                key_pos = first + lax.broadcasted_iota(jnp.int32, shape, 1)
                query_pos = start + lax.broadcasted_iota(jnp.int32, shape, 0)
                allowed = (key_pos <= query_pos) & (key_pos < valid)
                weight = jnp.concatenate(
                    [
                        jnp.where(allowed, weight[h * width : (h + 1) * width], 0.0)
                        for h in range(heads)
                    ],
                    axis=0,
                )
            total_ref[...] += jnp.dot(
                weight.astype(jnp.bfloat16),
                value_ext[pl.ds(first, span), :],
                preferred_element_type=jnp.float32,
            )

        full = jnp.minimum(start + 1, valid) // span
        stop = (jnp.minimum(start + width, valid) + span - 1) // span

        def plain(block, carry):
            step(block, False)
            return carry

        def edge(block, carry):
            step(block, True)
            return carry

        lax.fori_loop(0, full, plain, 0)
        lax.fori_loop(full, stop, edge, 0)
        live = start + lax.broadcasted_iota(jnp.int32, (width, HD), 0) < valid
        for h in range(heads):
            part = slice(h * width, (h + 1) * width)
            mixed = total_ref[part, :HD] / total_ref[part, HD:]
            out_ref[at_o + (slice(None), slice(h * HD, (h + 1) * HD))] = jnp.where(
                live, mixed, 0.0
            ).astype(jnp.bfloat16)


def attend_half(query, own, early, info, which):
    half, _, rows, size = query.shape
    part = half * rows
    span = min(512, part)
    return pl.pallas_call(
        functools.partial(attend_half_kernel, rows, span),
        grid_spec=pltpu.PrefetchScalarGridSpec(
            num_scalar_prefetch=1,
            grid=(half,),
            in_specs=[
                pl.BlockSpec((1, 1, rows, size), lambda i, _: (i, which, 0, 0)),
                pl.BlockSpec((half, 1, rows, 2 * HD), lambda i, _: (0, which, 0, 0)),
                pl.BlockSpec((half, rows, 2 * HD), lambda i, _: (0, 0, 0)),
            ],
            out_specs=pl.BlockSpec((1, rows, size), lambda i, _: (i, 0, 0)),
            scratch_shapes=[
                pltpu.VMEM((2 * part, HD), jnp.bfloat16),
                pltpu.VMEM((2 * part, 2 * HD), jnp.bfloat16),
                pltpu.VMEM((GROUP * rows, 2 * HD), jnp.float32),
            ],
        ),
        out_shape=jax.ShapeDtypeStruct((half, rows, size), jnp.bfloat16),
        cost_estimate=pl.CostEstimate(
            flops=6 * GROUP * part * part * HD,
            bytes_accessed=2 * part * HD * 8,
            transcendentals=GROUP * part * part,
        ),
        compiler_params=pltpu.CompilerParams(
            dimension_semantics=("arbitrary",), vmem_limit_bytes=40 * 1024 * 1024
        ),
    )(info, query, own, early)


def attend_kernel(heads, width, span, length_ref, packed_ref, out_ref, key_all, value_ext, total_ref):
    index = pl.program_id(0)
    count = packed_ref.shape[0]
    start = pl.multiple_of(index * width, width)

    @pl.when(index == 0)
    def _():
        key_all[...] = packed_ref[:, heads * HD : (heads + 1) * HD]
        value_ext[:, :HD] = packed_ref[:, (heads + 1) * HD :]
        value_ext[:, HD:] = jnp.ones((count, HD), jnp.bfloat16)

    query = packed_ref.at[pl.ds(start, width)]
    attend_block(
        heads, width, span, start, length_ref[0], query, (), key_all, value_ext, out_ref, (), total_ref
    )


def attend(packed, valid, heads):
    count = packed.shape[0]
    width = min(256, count)
    span = min(512, count)
    return pl.pallas_call(
        functools.partial(attend_kernel, heads, width, span),
        grid_spec=pltpu.PrefetchScalarGridSpec(
            num_scalar_prefetch=1,
            grid=(count // width,),
            in_specs=[pl.BlockSpec((count, (heads + 2) * HD), lambda i, _: (0, 0))],
            out_specs=pl.BlockSpec((width, heads * HD), lambda i, _: (i, 0)),
            scratch_shapes=[
                pltpu.VMEM((count, HD), jnp.bfloat16),
                pltpu.VMEM((count, 2 * HD), jnp.bfloat16),
                pltpu.VMEM((heads * width, 2 * HD), jnp.float32),
            ],
        ),
        out_shape=jax.ShapeDtypeStruct((count, heads * HD), jnp.bfloat16),
        cost_estimate=pl.CostEstimate(
            flops=4 * heads * count * count * HD,
            bytes_accessed=2 * count * HD * (2 * heads + 2),
            transcendentals=heads * count * count,
        ),
        compiler_params=pltpu.CompilerParams(
            dimension_semantics=("arbitrary",), vmem_limit_bytes=40 * 1024 * 1024
        ),
    )(valid, packed)


def pack_kernel(take, *refs):
    out_ref = refs[-1]
    for h in range(take):
        first = 0
        for ref in refs[:-1]:
            size = ref.shape[2] // take
            out_ref[h, :, first : first + size] = ref[0, :, h * size : (h + 1) * size]
            first += size


def pack(arrays, s):
    rows = arrays[0].shape[1]
    take = min(4, KVH)
    sizes = [a.shape[2] // KVH for a in arrays]
    total = sum(sizes)
    return pl.pallas_call(
        functools.partial(pack_kernel, take),
        grid=(KVH // take,),
        in_specs=[pl.BlockSpec((1, rows, take * size), lambda h: (s, 0, h)) for size in sizes],
        out_specs=pl.BlockSpec((take, rows, total), lambda h: (h, 0, 0)),
        out_shape=jax.ShapeDtypeStruct((KVH, rows, total), jnp.bfloat16),
        cost_estimate=pl.CostEstimate(
            flops=0, bytes_accessed=4 * KVH * rows * total, transcendentals=0
        ),
    )(*arrays)


def unpack_kernel(take, owned, *refs):
    out_ref = refs[-1]
    size = refs[0].shape[2]
    for d in range(take):
        for n, ref in enumerate(refs[:-1]):
            s, o = n // owned, n % owned
            first = (d * owned + o) * size
            out_ref[s, :, first : first + size] = ref[d]


def unpack(returned, owned):
    half, rows, size = returned[0].shape
    seqs = len(returned) // owned
    take = min(2, half)
    return pl.pallas_call(
        functools.partial(unpack_kernel, take, owned),
        grid=(half // take,),
        in_specs=[pl.BlockSpec((take, rows, size), lambda d: (d, 0, 0))] * len(returned),
        out_specs=pl.BlockSpec((seqs, rows, take * owned * size), lambda d: (0, 0, d)),
        out_shape=jax.ShapeDtypeStruct((seqs, rows, half * owned * size), jnp.bfloat16),
        cost_estimate=pl.CostEstimate(
            flops=0, bytes_accessed=4 * half * owned * seqs * rows * size, transcendentals=0
        ),
    )(*returned)


def exchange(array, groups=None):
    return lax.all_to_all(
        array, "tp", split_axis=0, concat_axis=0, tiled=True, axis_index_groups=groups
    )


def by_halves(queries, keys, values, lengths):
    seqs, rows, _ = queries.shape
    devices = lax.axis_size("tp")
    half = devices // 2
    owned = KVH // half
    groups = [list(range(half)), list(range(half, devices))]
    forward = [(j, half + j) for j in range(half)]
    base = jnp.where(lax.axis_index("tp") >= half, half * rows, 0).astype(jnp.int32)
    held = []
    for s in range(seqs):
        packed = pack((keys, values), s).reshape(half, owned * rows, -1)
        pair = exchange(packed, groups)
        pair = pair.reshape(half, owned, rows, -1)
        early = []
        for o in range(owned):
            part = pair[:, o]
            early.append(lax.ppermute(part, "tp", forward))
        packed = pack((queries,), s).reshape(half, owned * rows, -1)
        query = exchange(packed, groups)
        held.append((query.reshape(half, owned, rows, -1), pair, early))
    returned = []
    for s in range(seqs):
        query, pair, early = held[s]
        info = jnp.stack([lengths[s], base])
        for o in range(owned):
            returned.append(exchange(attend_half(query, pair, early[o], info, o), groups))
    return unpack(returned, owned)


def halves_fit(devices):
    return devices % 2 == 0 and KVH % (devices // 2) == 0


def per_device(queries, keys, values, lengths):
    seqs, rows, _ = queries.shape
    devices = lax.axis_size("tp")
    count = devices * rows
    if halves_fit(devices):
        return by_halves(queries, keys, values, lengths)

    pairs = seqs * HEADS
    owned = pairs // devices
    heads_q = queries.reshape(seqs, rows, HEADS, HD)
    heads_k = jnp.repeat(keys.reshape(seqs, rows, KVH, HD), GROUP, axis=2)
    heads_v = jnp.repeat(values.reshape(seqs, rows, KVH, HD), GROUP, axis=2)
    packed = jnp.concatenate([heads_q, heads_k, heads_v], axis=3)
    packed = packed.transpose(0, 2, 1, 3).reshape(devices, owned * rows, 3 * HD)
    gathered = exchange(packed).reshape(devices, owned, rows, 3 * HD)
    outs = []
    for o in range(owned):
        seq = (lax.axis_index("tp") * owned + o) // HEADS
        valid = jnp.sum(jnp.where(jnp.arange(seqs) == seq, lengths, 0))[None]
        outs.append(attend(gathered[:, o].reshape(count, 3 * HD), valid, 1))
    output = jnp.stack(outs).reshape(owned, devices, rows, HD).transpose(1, 0, 2, 3)
    returned = exchange(output.reshape(devices, owned * rows, HD))
    return (
        returned.reshape(seqs, HEADS, rows, HD)
        .transpose(0, 2, 1, 3)
        .reshape(seqs, rows, HEADS * HD)
    )


def solution(mesh):
    placed = (
        P("groups", "tp", None),
        P("groups", "tp", None),
        P("groups", "tp", None),
        P("groups"),
    )
    return jax.shard_map(
        per_device, mesh=mesh, in_specs=placed, out_specs=P("groups", "tp", None), check_vma=False
    )
```

```python
import functools
import math

import jax
import jax.numpy as jnp
from jax import lax
from jax.experimental import pallas as pl
from jax.experimental.pallas import tpu as pltpu
from jax.sharding import PartitionSpec as P


HEADS = 32
KVH = 16
HD = 128
GROUP = HEADS // KVH

SOFT_CAP = 50.0
SCORE_SCALE = 1.0 / (math.sqrt(144.0) * SOFT_CAP)
EXP_SCALE = SOFT_CAP * math.log2(math.e)


def attend_half_kernel(phase, width, span, info_ref, query_ref, *refs):
    refs = list(refs)
    own_ref = refs.pop(0) if phase != "early" else None
    early_ref = refs.pop(0) if phase != "own" else None
    begun_ref = refs.pop(0) if phase == "early" else None
    out_ref, key_all, value_ext, total_ref = refs
    index = pl.program_id(0)
    valid = info_ref[0]
    base = pl.multiple_of(info_ref[1], span)
    count = key_all.shape[0]
    start = base + index * width

    def hold(at, block):
        block = block.reshape(-1, 2 * HD)
        key_all[pl.ds(at, block.shape[0]), :] = block[:, :HD]
        value_ext[pl.ds(at, block.shape[0]), :HD] = block[:, HD:]

    @pl.when((index == 0) & (base < valid))
    def _():
        value_ext[:, HD:] = jnp.ones((count, HD), jnp.bfloat16)
        if phase == "both":
            hold(0, early_ref[...])
            hold(base, own_ref[:, 0])
        elif phase == "own":
            hold(0, own_ref[:, 0])
        else:
            hold(0, early_ref[...])

    attend_block(
        GROUP,
        width,
        span,
        start,
        valid,
        query_ref,
        (0, 0),
        key_all,
        value_ext,
        out_ref,
        (0,),
        total_ref,
        phase,
        base,
        begun_ref,
    )


def attend_block(
    heads,
    width,
    span,
    start,
    valid,
    query_ref,
    at_q,
    key_all,
    value_ext,
    out_ref,
    at_o,
    total_ref,
    phase="both",
    base=0,
    begun_ref=None,
):
    @pl.when(start >= valid)
    def _():
        out_ref[...] = jnp.zeros_like(out_ref)

    @pl.when(start < valid)
    def _():
        block_q = jnp.concatenate(
            [query_ref[at_q + (slice(None), slice(h * HD, (h + 1) * HD))] for h in range(heads)],
            axis=0,
        )
        if phase == "early":
            total_ref[...] = begun_ref[0]
        else:
            total_ref[...] = jnp.zeros_like(total_ref)
        shift = base if phase == "own" else 0

        def step(block, masked):
            first = pl.multiple_of(block * span, span)
            held = pl.ds(pl.multiple_of(first - shift, span), span)
            score = lax.dot_general(
                block_q,
                key_all[held, :],
                (((1,), (1,)), ((), ())),
                preferred_element_type=jnp.float32,
            )
            weight = jnp.exp2(jnp.tanh(score * SCORE_SCALE) * EXP_SCALE)
            if masked:
                shape = (width, span)
                key_pos = first + lax.broadcasted_iota(jnp.int32, shape, 1)
                query_pos = start + lax.broadcasted_iota(jnp.int32, shape, 0)
                allowed = (key_pos <= query_pos) & (key_pos < valid)
                weight = jnp.concatenate(
                    [
                        jnp.where(allowed, weight[h * width : (h + 1) * width], 0.0)
                        for h in range(heads)
                    ],
                    axis=0,
                )
            total_ref[...] += jnp.dot(
                weight.astype(jnp.bfloat16),
                value_ext[held, :],
                preferred_element_type=jnp.float32,
            )

        full = jnp.minimum(start + 1, valid) // span
        stop = (jnp.minimum(start + width, valid) + span - 1) // span

        def plain(block, carry):
            step(block, False)
            return carry

        def edge(block, carry):
            step(block, True)
            return carry

        if phase == "early":
            lax.fori_loop(0, base // span, plain, 0)
        else:
            lax.fori_loop(shift // span, full, plain, 0)
            lax.fori_loop(full, stop, edge, 0)
        if phase == "own":
            out_ref[0] = total_ref[...]
            return
        live = start + lax.broadcasted_iota(jnp.int32, (width, HD), 0) < valid
        for h in range(heads):
            part = slice(h * width, (h + 1) * width)
            mixed = total_ref[part, :HD] / total_ref[part, HD:]
            out_ref[at_o + (slice(None), slice(h * HD, (h + 1) * HD))] = jnp.where(
                live, mixed, 0.0
            ).astype(jnp.bfloat16)


def attend_half(query, own, early, begun, info, which):
    half, _, rows, size = query.shape
    part = half * rows
    span = min(512, part)
    phase = "own" if early is None else "both" if begun is None else "early"
    held = part if phase != "both" else 2 * part
    specs = [pl.BlockSpec((1, 1, rows, size), lambda i, _: (i, which, 0, 0))]
    whole = pl.BlockSpec((half, 1, rows, 2 * HD), lambda i, _: (0, 0, 0, 0))
    sums = pl.BlockSpec((1, GROUP * rows, 2 * HD), lambda i, _: (i, 0, 0))
    arrays = [query]
    if phase != "early":
        specs.append(whole)
        arrays.append(own)
    if phase != "own":
        specs.append(pl.BlockSpec((half, rows, 2 * HD), lambda i, _: (0, 0, 0)))
        arrays.append(early)
    if phase == "early":
        specs.append(sums)
        arrays.append(begun)
    if phase == "own":
        out_spec = sums
        out_shape = jax.ShapeDtypeStruct((half, GROUP * rows, 2 * HD), jnp.float32)
    else:
        out_spec = pl.BlockSpec((1, rows, size), lambda i, _: (i, 0, 0))
        out_shape = jax.ShapeDtypeStruct((half, rows, size), jnp.bfloat16)
    work = {"own": 2, "early": 4, "both": 6}[phase]
    return pl.pallas_call(
        functools.partial(attend_half_kernel, phase, rows, span),
        grid_spec=pltpu.PrefetchScalarGridSpec(
            num_scalar_prefetch=1,
            grid=(half,),
            in_specs=specs,
            out_specs=out_spec,
            scratch_shapes=[
                pltpu.VMEM((held, HD), jnp.bfloat16),
                pltpu.VMEM((held, 2 * HD), jnp.bfloat16),
                pltpu.VMEM((GROUP * rows, 2 * HD), jnp.float32),
            ],
        ),
        out_shape=out_shape,
        cost_estimate=pl.CostEstimate(
            flops=work * GROUP * part * part * HD,
            bytes_accessed=2 * part * HD * 8,
            transcendentals=GROUP * part * part,
        ),
        compiler_params=pltpu.CompilerParams(
            dimension_semantics=("arbitrary",), vmem_limit_bytes=40 * 1024 * 1024
        ),
    )(info, *arrays)


def attend_kernel(heads, width, span, length_ref, packed_ref, out_ref, key_all, value_ext, total_ref):
    index = pl.program_id(0)
    count = packed_ref.shape[0]
    start = pl.multiple_of(index * width, width)

    @pl.when(index == 0)
    def _():
        key_all[...] = packed_ref[:, heads * HD : (heads + 1) * HD]
        value_ext[:, :HD] = packed_ref[:, (heads + 1) * HD :]
        value_ext[:, HD:] = jnp.ones((count, HD), jnp.bfloat16)

    query = packed_ref.at[pl.ds(start, width)]
    attend_block(
        heads, width, span, start, length_ref[0], query, (), key_all, value_ext, out_ref, (), total_ref
    )


def attend(packed, valid, heads):
    count = packed.shape[0]
    width = min(256, count)
    span = min(512, count)
    return pl.pallas_call(
        functools.partial(attend_kernel, heads, width, span),
        grid_spec=pltpu.PrefetchScalarGridSpec(
            num_scalar_prefetch=1,
            grid=(count // width,),
            in_specs=[pl.BlockSpec((count, (heads + 2) * HD), lambda i, _: (0, 0))],
            out_specs=pl.BlockSpec((width, heads * HD), lambda i, _: (i, 0)),
            scratch_shapes=[
                pltpu.VMEM((count, HD), jnp.bfloat16),
                pltpu.VMEM((count, 2 * HD), jnp.bfloat16),
                pltpu.VMEM((heads * width, 2 * HD), jnp.float32),
            ],
        ),
        out_shape=jax.ShapeDtypeStruct((count, heads * HD), jnp.bfloat16),
        cost_estimate=pl.CostEstimate(
            flops=4 * heads * count * count * HD,
            bytes_accessed=2 * count * HD * (2 * heads + 2),
            transcendentals=heads * count * count,
        ),
        compiler_params=pltpu.CompilerParams(
            dimension_semantics=("arbitrary",), vmem_limit_bytes=40 * 1024 * 1024
        ),
    )(valid, packed)


def pack_kernel(take, owned, *refs):
    count = len(refs) - owned
    for h in range(take):
        out_ref = refs[count + h % owned]
        first = 0
        for ref in refs[:count]:
            size = ref.shape[2] // take
            out_ref[h // owned, :, first : first + size] = ref[0, :, h * size : (h + 1) * size]
            first += size


def pack(arrays, s, owned):
    rows = arrays[0].shape[1]
    take = min(4, KVH) // owned * owned
    sizes = [a.shape[2] // KVH for a in arrays]
    total = sum(sizes)
    shape = jax.ShapeDtypeStruct((KVH // owned, rows, total), jnp.bfloat16)
    return pl.pallas_call(
        functools.partial(pack_kernel, take, owned),
        grid=(KVH // take,),
        in_specs=[pl.BlockSpec((1, rows, take * size), lambda h: (s, 0, h)) for size in sizes],
        out_specs=[pl.BlockSpec((take // owned, rows, total), lambda h: (h, 0, 0))] * owned,
        out_shape=[shape] * owned,
        cost_estimate=pl.CostEstimate(
            flops=0, bytes_accessed=4 * KVH * rows * total, transcendentals=0
        ),
    )(*arrays)


def unpack_kernel(take, owned, *refs):
    out_ref = refs[-1]
    size = refs[0].shape[3]
    for d in range(take):
        for n, ref in enumerate(refs[:-1]):
            s, o = n // owned, n % owned
            first = (d * owned + o) * size
            out_ref[s, :, first : first + size] = ref[d, 0]


def unpack(returned, places, owned):
    half, _, rows, size = returned[0].shape
    seqs = len(returned) // owned
    take = min(2, half)
    return pl.pallas_call(
        functools.partial(unpack_kernel, take, owned),
        grid=(half // take,),
        in_specs=[
            pl.BlockSpec((take, 1, rows, size), lambda d, o=o: (d, o, 0, 0)) for o in places
        ],
        out_specs=pl.BlockSpec((seqs, rows, take * owned * size), lambda d: (0, 0, d)),
        out_shape=jax.ShapeDtypeStruct((seqs, rows, half * owned * size), jnp.bfloat16),
        cost_estimate=pl.CostEstimate(
            flops=0, bytes_accessed=4 * half * owned * seqs * rows * size, transcendentals=0
        ),
    )(*returned)


def exchange(array, groups=None):
    return lax.all_to_all(
        array, "tp", split_axis=0, concat_axis=0, tiled=True, axis_index_groups=groups
    )


def by_halves(queries, keys, values, lengths):
    seqs, rows, _ = queries.shape
    devices = lax.axis_size("tp")
    half = devices // 2
    owned = KVH // half
    groups = [list(range(half)), list(range(half, devices))]
    forward = [(j, half + j) for j in range(half)]
    base = jnp.where(lax.axis_index("tp") >= half, half * rows, 0).astype(jnp.int32)
    held = []
    for s in range(seqs):
        pairs, early = [], []
        for o, packed in enumerate(pack((keys, values), s, owned)):
            pairs.append(exchange(packed, groups))
            early.append(lax.ppermute(pairs[o], "tp", forward))
        packed = pack((queries,), s, 1)[0].reshape(half, owned * rows, -1)
        query = exchange(packed, groups)
        held.append((query.reshape(half, owned, rows, -1), pairs, early))
    returned, places = [], []
    for s in range(seqs):
        query, pairs, early = held[s]
        info = jnp.stack([lengths[s], base])
        outs = []
        for o in range(owned):
            pair, begun = pairs[o][:, None], None
            if s == seqs - 1 and o == owned - 1:
                begun = attend_half(query, pair, None, None, info, o)
            outs.append(attend_half(query, pair, early[o], begun, info, o))
        if s < seqs - 1:
            output = jnp.stack(outs, axis=1).reshape(half, owned * rows, -1)
            back = exchange(output, groups).reshape(half, owned, rows, -1)
            returned += [back] * owned
            places += range(owned)
        else:
            returned += [exchange(output, groups)[:, None] for output in outs]
            places += [0] * owned
    return unpack(returned, places, owned)


def halves_fit(devices):
    return devices % 2 == 0 and KVH % (devices // 2) == 0


def per_device(queries, keys, values, lengths):
    seqs, rows, _ = queries.shape
    devices = lax.axis_size("tp")
    count = devices * rows
    if halves_fit(devices):
        return by_halves(queries, keys, values, lengths)

    pairs = seqs * HEADS
    owned = pairs // devices
    heads_q = queries.reshape(seqs, rows, HEADS, HD)
    heads_k = jnp.repeat(keys.reshape(seqs, rows, KVH, HD), GROUP, axis=2)
    heads_v = jnp.repeat(values.reshape(seqs, rows, KVH, HD), GROUP, axis=2)
    packed = jnp.concatenate([heads_q, heads_k, heads_v], axis=3)
    packed = packed.transpose(0, 2, 1, 3).reshape(devices, owned * rows, 3 * HD)
    gathered = exchange(packed).reshape(devices, owned, rows, 3 * HD)
    outs = []
    for o in range(owned):
        seq = (lax.axis_index("tp") * owned + o) // HEADS
        valid = jnp.sum(jnp.where(jnp.arange(seqs) == seq, lengths, 0))[None]
        outs.append(attend(gathered[:, o].reshape(count, 3 * HD), valid, 1))
    output = jnp.stack(outs).reshape(owned, devices, rows, HD).transpose(1, 0, 2, 3)
    returned = exchange(output.reshape(devices, owned * rows, HD))
    return (
        returned.reshape(seqs, HEADS, rows, HD)
        .transpose(0, 2, 1, 3)
        .reshape(seqs, rows, HEADS * HD)
    )


def solution(mesh):
    placed = (
        P("groups", "tp", None),
        P("groups", "tp", None),
        P("groups", "tp", None),
        P("groups"),
    )
    return jax.shard_map(
        per_device, mesh=mesh, in_specs=placed, out_specs=P("groups", "tp", None), check_vma=False
    )
```
